8 devices in a mesh: rep: 2 (over y, z), dp: 4 (over x, core).
Axes of the slice: x: 2, y: 2, z: 1, core: 2. Of those that a mesh axis runs over, the one named last changes fastest.
Arguments:
- a: bfloat16 [8, 4, 4096, 1024], P(('rep', 'dp')), parts along dimension 0
- g: bfloat16 [8, 4, 4096, 3200], P(('rep', 'dp')), parts along dimension 0
Outputs:
- output: bfloat16 [8, 1024, 3200], P('rep'), parts along dimension 0
There are 2 independent parts. The reference program is written for one: setup_inputs(seed, part) draws one part's arguments, and reference() takes and returns one part's arrays. A program takes and returns all parts, laid end to end along the dimension named above; each array names one.
All inputs are finite; a program needn't handle non-finite values.
Results may differ from the reference program's by a relative error of at most 0.012.
Values are sent between devices in bfloat16 or wider.
A program may use at most 2 GiB of HBM per device.

```python
import jax
import jax.numpy as jnp
from jax import lax

DEVICES = 4
MATRICES = 4
TOKENS = 4096
D = 1024
FF = 3200


def setup_inputs(seed: int = 0, part: int = 0) -> dict:
    ka, kg, ks = (jax.random.fold_in(k, part) for k in jax.random.split(jax.random.key(seed), 3))
    size = 2.0 ** jax.random.uniform(ks, (DEVICES, MATRICES, 1, 1), jnp.float32, -1.0, 1.0)
    a = jax.random.normal(ka, (DEVICES, MATRICES, TOKENS, D), jnp.float32)
    g = size * jax.random.normal(kg, (DEVICES, MATRICES, TOKENS, FF), jnp.float32) * (DEVICES * TOKENS) ** -0.5
    return {"a": a.astype(jnp.bfloat16), "g": g.astype(jnp.bfloat16)}


def reference(a, g):
    def take(so_far, one):
        return so_far + jnp.einsum("ntd,ntf->ndf", *one, preferred_element_type=jnp.float32), None

    return lax.scan(take, jnp.zeros((MATRICES, D, FF), jnp.float32), (a, g))[0].astype(jnp.bfloat16)
```

```python
import functools

import jax
import jax.numpy as jnp
from jax import lax
from jax.experimental import pallas as pl
from jax.experimental.pallas import tpu as pltpu
from jax.sharding import PartitionSpec as P

MESH = pl.DeviceIdType.MESH
WIDTH = 640
LAG = 2
LAG2 = 2 * LAG + 1
RING = 4


def kernel(
    a, g, out, abuf, gbuf, sb1, rv1, mine, sb2, rv2, fin,
    asem, gsem, s1, r1, s2, r2, local, s3, r3, s4, r4, s5, r5,
):
    _, mats, tokens, dim = a.shape
    quarter = dim // 4
    per = g.shape[3] // WIDTH
    chunks = mats * per
    rep, dp = lax.axis_index("rep"), lax.axis_index("dp")
    partner = 2 * (dp // 2) + 1 - dp % 2
    peer = (dp + 2) % 4
    peers_partner = 3 - dp
    order = (peers_partner, partner, peer, dp)

    def rows(q):
        return pl.ds(pl.multiple_of(q * quarter, quarter), quarter)

    def place(k, q):
        return out.at[k // per, rows(q), pl.ds(pl.multiple_of((k % per) * WIDTH, 128), WIDTH)]

    def load_a(n, i):
        return pltpu.make_async_copy(
            a.at[0, n, :, rows(order[i])], abuf.at[n % 2, :, rows(order[i])], asem.at[n % 2, i])

    def load_g(k):
        cols = pl.ds(pl.multiple_of((k % per) * WIDTH, 128), WIDTH)
        return pltpu.make_async_copy(g.at[0, k // per, :, cols], gbuf.at[k % 2], gsem.at[k % 2])

    def remote(src, dst, send, recv, to):
        return pltpu.make_async_remote_copy(
            src_ref=src, dst_ref=dst, send_sem=send, recv_sem=recv,
            device_id=(rep, to), device_id_type=MESH)

    def term(k, i):
        return remote(sb1.at[k % 2, i], rv1.at[k, i], s1.at[k % 2, i], r1.at[k, i], partner)

    def half(k):
        return remote(sb2.at[k % RING], rv2.at[k], s2.at[k % RING], r2.at[k], peer)

    def keep(k):
        return pltpu.make_async_copy(fin.at[k % RING], place(k, dp), local.at[k % RING])

    def give(k):
        return remote(fin.at[k % RING], place(k, dp), s3.at[k % RING], r3.at[k], partner)

    def cross(k):
        return remote(fin.at[k % RING], place(k, dp), s4.at[k % RING], r4.at[k], peer)

    def forward(k):
        return remote(place(k, peer), place(k, peer), s5.at[k], r5.at[k], partner)

    def product(k, i):
        left = abuf[(k // per) % 2, :, rows(order[i])]
        return lax.dot_general(left, gbuf[k % 2], (((0,), (0,)), ((), ())), preferred_element_type=jnp.float32)

    def multiply(k):
        n = k // per
        first = k % per == 0

        @pl.when(k + 1 < chunks)
        def _():
            load_g(k + 1).start()

        @pl.when(first & (n + 1 < mats))
        def _():
            for i in range(4):
                load_a(n + 1, i).start()

        load_g(k).wait()

        def ready(i):
            @pl.when(first)
            def _():
                load_a(n, i).wait()

        for i in range(2):
            @pl.when(k >= 2)
            def _():
                term(k - 2, i).wait_send()

            ready(i)
            sb1[k % 2, i] = product(k, i).astype(jnp.bfloat16)
            term(k, i).start()
        ready(2)
        total = product(k, 2)
        term(k, 0).wait_recv()

        @pl.when(k >= RING)
        def _():
            half(k - RING).wait_send()

        sb2[k % RING] = (total + rv1[k, 0].astype(jnp.float32)).astype(jnp.bfloat16)
        half(k).start()
        ready(3)
        total = product(k, 3)
        term(k, 1).wait_recv()
        mine[k % (LAG + 1)] = total + rv1[k, 1].astype(jnp.float32)

    def finish(k):
        half(k).wait_recv()

        @pl.when(k >= RING)
        def _():
            keep(k - RING).wait()
            give(k - RING).wait_send()
            cross(k - RING).wait_send()

        fin[k % RING] = (mine[k % (LAG + 1)] + rv2[k].astype(jnp.float32)).astype(jnp.bfloat16)
        cross(k).start()
        give(k).start()
        keep(k).start()

    def hand_on(k):
        cross(k).wait_recv()
        forward(k).start()

    load_a(0, 0).start()
    load_g(0).start()
    for i in range(1, 4):
        load_a(0, i).start()
    barrier = pltpu.get_barrier_semaphore()
    for other in (partner, peer):
        pl.semaphore_signal(barrier, inc=1, device_id=(rep, other), device_id_type=MESH)
    pl.semaphore_wait(barrier, 2)

    def step(k, _):
        @pl.when(k < chunks)
        def _():
            multiply(k)

        @pl.when((k >= LAG) & (k < chunks + LAG))
        def _():
            finish(k - LAG)

        @pl.when(k >= LAG2)
        def _():
            hand_on(k - LAG2)

    lax.fori_loop(0, chunks + LAG2, step, None)

    def drain(k, _):
        give(k).wait_recv()
        forward(k).wait()

    for k in range(chunks - 2, chunks):
        for i in range(2):
            term(k, i).wait_send()
    for k in range(chunks - RING, chunks):
        half(k).wait_send()
        keep(k).wait()
        give(k).wait_send()
        cross(k).wait_send()
    lax.fori_loop(0, chunks, drain, None)


def solution(mesh):
    def step(a, g):
        _, mats, tokens, dim = a.shape
        wide = g.shape[3]
        chunks = mats * (wide // WIDTH)
        block = (dim // 4, WIDTH)
        dma = pltpu.SemaphoreType.DMA
        bf16, f32 = jnp.bfloat16, jnp.float32
        return pl.pallas_call(
            kernel,
            out_shape=jax.ShapeDtypeStruct((mats, dim, wide), bf16),
            in_specs=[pl.BlockSpec(memory_space=pl.ANY)] * 2,
            out_specs=pl.BlockSpec(memory_space=pl.ANY),
            scratch_shapes=[
                pltpu.VMEM((2, tokens, dim), bf16),
                pltpu.VMEM((2, tokens, WIDTH), bf16),
                pltpu.VMEM((2, 2, *block), bf16),
                pltpu.VMEM((chunks, 2, *block), bf16),
                pltpu.VMEM((LAG + 1, *block), f32),
                pltpu.VMEM((RING, *block), bf16),
                pltpu.VMEM((chunks, *block), bf16),
                pltpu.VMEM((RING, *block), bf16),
                dma((2, 4)), dma((2,)),
                dma((2, 2)), dma((chunks, 2)),
                dma((RING,)), dma((chunks,)),
                dma((RING,)),
                dma((RING,)), dma((chunks,)),
                dma((RING,)), dma((chunks,)),
                dma((chunks,)), dma((chunks,)),
            ],
            compiler_params=pltpu.CompilerParams(
                collective_id=0, has_side_effects=True, vmem_limit_bytes=66_000_000),
        )(a, g)

    both = P(("rep", "dp"))
    return jax.shard_map(step, mesh=mesh, in_specs=(both, both), out_specs=P("rep"), check_vma=False)
```

```python
import jax
import jax.numpy as jnp
from jax import lax
from jax.experimental import pallas as pl
from jax.experimental.pallas import tpu as pltpu
from jax.sharding import PartitionSpec as P

MESH = pl.DeviceIdType.MESH
WIDTH = 640
RING = 4
PIECES = ((0, 128, 0, 256), (128, 128, 0, 256), (0, 256, 256, 256), (0, 256, 512, 128))


def kernel(
    a, g, out, abuf, gbuf, sb1, rv1, total, sb2, rv2,
    asem, hsem, gsem, g0sem, s1, r1, p1, q1, s2, r2, p2, q2, s3, r3, s4, r4, s5, r5,
):
    _, mats, tokens, dim = a.shape
    quarter = dim // 4
    per = g.shape[3] // WIDTH
    chunks = mats * per
    rep, dp = lax.axis_index("rep"), lax.axis_index("dp")
    partner = 2 * (dp // 2) + 1 - dp % 2
    peer = (dp + 2) % 4
    order = (3 - dp, partner, peer, dp)

    def rows(q, start=0, size=quarter):
        return pl.ds(pl.multiple_of(q * quarter + start, 128), size)

    def columns(k):
        return pl.ds(pl.multiple_of((k % per) * WIDTH, 128), WIDTH)

    def place(k, q):
        return out.at[k, rows(q)]

    def load_a(n, i):
        return pltpu.make_async_copy(
            a.at[0, n, :, rows(order[i])], abuf.at[n % 2, :, rows(order[i])], asem.at[n % 2, i])

    def load_half(i, h):
        part = rows(order[i], h * 128, 128)
        return pltpu.make_async_copy(a.at[0, 0, :, part], abuf.at[0, :, part], hsem.at[i // 2, h])

    def load_g(k):
        return pltpu.make_async_copy(g.at[0, k // per, :, columns(k)], gbuf.at[k % 3], gsem.at[k % 3])

    def load_g0(j, start, size):
        part = pl.ds(start, size)
        return pltpu.make_async_copy(g.at[0, 0, :, part], gbuf.at[0, :, part], g0sem.at[j])

    def remote(src, dst, send, recv, to):
        return pltpu.make_async_remote_copy(
            src_ref=src, dst_ref=dst, send_sem=send, recv_sem=recv,
            device_id=(rep, to), device_id_type=MESH)

    def term(k, i):
        return remote(sb1.at[k % 2, i], rv1.at[k % 2, i], s1.at[k % 2, i], r1.at[k, i], partner)

    def term_piece(j):
        r, h, c, w = PIECES[j]
        part = (pl.ds(r, h), pl.ds(c, w))
        return remote(sb1.at[0, 0, *part], rv1.at[0, 0, *part], p1.at[j], q1.at[j], partner)

    def half(k):
        return remote(sb2.at[k % 2], rv2.at[k % RING], s2.at[k % 2], r2.at[k], peer)

    def half_piece(j):
        r, h, c, w = PIECES[j]
        part = (pl.ds(r, h), pl.ds(c, w))
        return remote(sb2.at[0, *part], rv2.at[0, *part], p2.at[j], q2.at[j], peer)

    def give(k):
        return remote(place(k, dp), place(k, dp), s3.at[k], r3.at[k], partner)

    def cross(k):
        return remote(place(k, dp), place(k, dp), s4.at[k], r4.at[k], peer)

    def forward(k):
        return remote(place(k, peer), place(k, peer), s5.at[k], r5.at[k], partner)

    def dot(left, right):
        return lax.dot_general(left, right, (((0,), (0,)), ((), ())), preferred_element_type=jnp.float32)

    def product(k, i):
        return dot(abuf[(k // per) % 2, :, rows(order[i])], gbuf[k % 3])

    def both(here, there):
        return here + there.astype(jnp.float32)

    def first_part():
        def piece(j, i):
            r, h, c, w = PIECES[j]
            return dot(abuf[0, :, rows(order[i], r, h)], gbuf[0, :, c:c + w])

        def send(j):
            r, h, c, w = PIECES[j]
            term_piece(j).wait_recv()
            sb2[0, r:r + h, c:c + w] = both(total[r:r + h, c:c + w], rv1[0, 0, r:r + h, c:c + w]).astype(jnp.bfloat16)
            half_piece(j).start()

        for j, (r, h, c, w) in enumerate(PIECES):
            if j == 0:
                load_half(0, 0).wait()
                load_g0(0, 0, 256).wait()
            if j == 1:
                load_half(0, 1).wait()
            if j == 2:
                load_g0(1, 256, 384).wait()
            sb1[0, 0, r:r + h, c:c + w] = piece(j, 0).astype(jnp.bfloat16)
            term_piece(j).start()
            if j:
                send(j - 1)
            if j < 2:
                load_half(2, j).wait()
            total[r:r + h, c:c + w] = piece(j, 2)
            if j == 0:
                load_g(1).start()
                load_a(0, 1).start()
                load_a(0, 3).start()
        send(len(PIECES) - 1)
        load_g(2).start()
        for i in range(4):
            load_a(1, i).start()

    def reduce_part(k):
        first = k % per == 0
        load_g(k).wait()

        @pl.when(first)
        def _():
            load_a(k // per, 0).wait()
            load_a(k // per, 2).wait()

        @pl.when(k == 2)
        def _():
            for j in range(len(PIECES)):
                term_piece(j).wait_send()

        @pl.when(k > 2)
        def _():
            term(k - 2, 0).wait_send()

        sb1[k % 2, 0] = product(k, 0).astype(jnp.bfloat16)
        term(k, 0).start()
        total[...] = product(k, 2)
        term(k, 0).wait_recv()

        @pl.when(k == 2)
        def _():
            for j in range(len(PIECES)):
                half_piece(j).wait_send()

        @pl.when(k > 2)
        def _():
            half(k - 2).wait_send()

        sb2[k % 2] = both(total[...], rv1[k % 2, 0]).astype(jnp.bfloat16)
        half(k).start()

    def owner_part(k):
        @pl.when(k % per == 0)
        def _():
            load_a(k // per, 1).wait()
            load_a(k // per, 3).wait()

        @pl.when(k >= 2)
        def _():
            term(k - 2, 1).wait_send()

        sb1[k % 2, 1] = product(k, 1).astype(jnp.bfloat16)
        term(k, 1).start()
        total[...] = product(k, 3)

        @pl.when(k + 3 < chunks)
        def _():
            load_g(k + 3).start()

        @pl.when((k % per == per - 1) & (k // per + 2 < mats))
        def _():
            for i in range(4):
                load_a(k // per + 2, i).start()

        term(k, 1).wait_recv()

        @pl.when(k == 0)
        def _():
            for j in range(len(PIECES)):
                half_piece(j).wait_recv()

        @pl.when(k > 0)
        def _():
            half(k).wait_recv()

        out[k, rows(dp)] = both(both(total[...], rv1[k % 2, 1]), rv2[k % RING]).astype(jnp.bfloat16)
        cross(k).start()
        give(k).start()

    load_half(0, 0).start()
    load_g0(0, 0, 256).start()
    load_half(2, 0).start()
    load_half(0, 1).start()
    load_half(2, 1).start()
    load_g0(1, 256, 384).start()
    barrier = pltpu.get_barrier_semaphore()
    for other in (partner, peer):
        pl.semaphore_signal(barrier, inc=1, device_id=(rep, other), device_id_type=MESH)
    pl.semaphore_wait(barrier, 2)
    first_part()

    def step(k, _):
        @pl.when(k + 1 < chunks)
        def _():
            reduce_part(k + 1)

        @pl.when(k < chunks)
        def _():
            owner_part(k)

        @pl.when(k >= 2)
        def _():
            cross(k - 2).wait_recv()
            forward(k - 2).start()

    lax.fori_loop(0, chunks + 2, step, None)

    for k in range(chunks - 2, chunks):
        for i in range(2):
            term(k, i).wait_send()
        half(k).wait_send()

    def drain(k, _):
        cross(k).wait_send()
        give(k).wait()
        forward(k).wait()

    lax.fori_loop(0, chunks, drain, None)


def write(done, out, sem):
    chunks = done.shape[0]
    per = chunks // out.shape[0]

    def copy(k):
        return pltpu.make_async_copy(done.at[k], out.at[k // per, :, pl.ds((k % per) * WIDTH, WIDTH)], sem.at[k])

    for k in range(chunks):
        copy(k).start()
    for k in range(chunks):
        copy(k).wait()


def solution(mesh):
    def step(a, g):
        _, mats, tokens, dim = a.shape
        wide = g.shape[3]
        chunks = mats * (wide // WIDTH)
        block = (dim // 4, WIDTH)
        dma = pltpu.SemaphoreType.DMA
        bf16, f32 = jnp.bfloat16, jnp.float32
        pieces = len(PIECES)
        done = pl.pallas_call(
            kernel,
            out_shape=pltpu.VMEM((chunks, dim, WIDTH), bf16),
            in_specs=[pl.BlockSpec(memory_space=pl.ANY)] * 2,
            out_specs=pl.BlockSpec(memory_space=pltpu.VMEM),
            scratch_shapes=[
                pltpu.VMEM((2, tokens, dim), bf16),
                pltpu.VMEM((3, tokens, WIDTH), bf16),
                pltpu.VMEM((2, 2, *block), bf16),
                pltpu.VMEM((2, 2, *block), bf16),
                pltpu.VMEM(block, f32),
                pltpu.VMEM((2, *block), bf16),
                pltpu.VMEM((RING, *block), bf16),
                dma((2, 4)), dma((2, 2)), dma((3,)), dma((2,)),
                dma((2, 2)), dma((chunks, 2)), dma((pieces,)), dma((pieces,)),
                dma((2,)), dma((chunks,)), dma((pieces,)), dma((pieces,)),
                dma((chunks,)), dma((chunks,)),
                dma((chunks,)), dma((chunks,)),
                dma((chunks,)), dma((chunks,)),
            ],
            compiler_params=pltpu.CompilerParams(
                collective_id=0, has_side_effects=True, vmem_limit_bytes=40_700_000),
            name="reduce",
        )(a, g)
        return pl.pallas_call(
            write,
            out_shape=jax.ShapeDtypeStruct((mats, dim, wide), bf16),
            in_specs=[pl.BlockSpec(memory_space=pltpu.VMEM)],
            out_specs=pl.BlockSpec(memory_space=pl.ANY),
            scratch_shapes=[dma((chunks,))],
            compiler_params=pltpu.CompilerParams(vmem_limit_bytes=1_000_000),
            name="write",
        )(done)

    both = P(("rep", "dp"))
    return jax.shard_map(step, mesh=mesh, in_specs=(both, both), out_specs=P("rep"), check_vma=False)
```

```python
import functools

import jax
import jax.numpy as jnp
from jax import lax
from jax.experimental import pallas as pl
from jax.experimental.pallas import tpu as pltpu
from jax.sharding import PartitionSpec as P


MESH = pl.DeviceIdType.MESH
WIDTH = 640
RING = 4
PIECES = ((0, 128, 0, 256), (128, 128, 0, 256), (0, 256, 256, 384))
LAST = 2
TAIL = 128


def kernel(
    a, g, out, got, la, lb, abuf, gbuf, sb1, rv1, total, sb2, rv2,
    asem, hsem, gsem, g0sem, s1, r1, p1, q1, s2, r2, p2, q2, s3, r3, s4, r4, s5, r5,
):
    _, mats, _, dim = a.shape
    quarter = dim // 4
    per = g.shape[3] // WIDTH
    chunks = mats * per
    inside = chunks - LAST
    rep, dp = lax.axis_index("rep"), lax.axis_index("dp")
    partner = 2 * (dp // 2) + 1 - dp % 2
    peer = (dp + 2) % 4
    order = (3 - dp, partner, peer, dp)

    def rows(q, start=0, size=quarter):
        return pl.ds(pl.multiple_of(q * quarter + start, 128), size)

    def columns(k):
        return pl.ds(pl.multiple_of((k % per) * WIDTH, 128), WIDTH)

    def place(k, q):
        return out.at[k, rows(q)]

    def load_a(n, i):
        return pltpu.make_async_copy(
            a.at[0, n, :, rows(order[i])], abuf.at[:, rows(order[i])], asem.at[i])

    def load_half(i, h):
        part = rows(order[i], h * 128, 128)
        return pltpu.make_async_copy(a.at[0, 0, :, part], abuf.at[:, part], hsem.at[i // 2, h])

    def load_g(k):
        return pltpu.make_async_copy(g.at[0, k // per, :, columns(k)], gbuf.at[k % 3], gsem.at[k % 3])

    def load_g0(j, start, size):
        part = pl.ds(start, size)
        return pltpu.make_async_copy(g.at[0, 0, :, part], gbuf.at[0, :, part], g0sem.at[j])

    def remote(src, dst, send, recv, to):
        return pltpu.make_async_remote_copy(
            src_ref=src, dst_ref=dst, send_sem=send, recv_sem=recv,
            device_id=(rep, to), device_id_type=MESH)

    def term(k, i):
        return remote(sb1.at[k % 2, i], rv1.at[k % 2, i], s1.at[k % 2, i], r1.at[k, i], partner)

    def term_piece(j):
        r, h, c, w = PIECES[j]
        part = (pl.ds(r, h), pl.ds(c, w))
        return remote(sb1.at[0, 0, *part], rv1.at[0, 0, *part], p1.at[j], q1.at[j], partner)

    def half(k):
        return remote(sb2.at[k % 2], rv2.at[k % RING], s2.at[k % 2], r2.at[k], peer)

    def half_piece(j):
        r, h, c, w = PIECES[j]
        part = (pl.ds(r, h), pl.ds(c, w))
        return remote(sb2.at[0, *part], rv2.at[0, *part], p2.at[j], q2.at[j], peer)

    def give(k):
        return remote(place(k, dp), place(k, dp), s3.at[k], r3.at[k], partner)

    def cross(k):
        return remote(place(k, dp), place(k, dp), s4.at[k], r4.at[k], peer)

    def cross_last():
        return remote(place(inside - 1, dp), got, s4.at[inside - 1], r4.at[inside - 1], peer)

    def forward(k):
        return remote(place(k, peer), place(k, peer), s5.at[k], r5.at[k], partner)

    def dot(left, right):
        return lax.dot_general(left, right, (((0,), (0,)), ((), ())), preferred_element_type=jnp.float32)

    def product(k, i):
        return dot(abuf[:, rows(order[i])], gbuf[k % 3])

    def both(here, there):
        return here + there.astype(jnp.float32)

    def first_part():
        def piece(j, i):
            r, h, c, w = PIECES[j]
            return dot(abuf[:, rows(order[i], r, h)], gbuf[0, :, c:c + w])

        def send(j):
            r, h, c, w = PIECES[j]
            term_piece(j).wait_recv()
            sb2[0, r:r + h, c:c + w] = both(total[r:r + h, c:c + w], rv1[0, 0, r:r + h, c:c + w]).astype(jnp.bfloat16)
            half_piece(j).start()

        for j, (r, h, c, w) in enumerate(PIECES):
            if j == 0:
                load_half(0, 0).wait()
                load_g0(0, 0, 256).wait()
            if j == 1:
                load_half(0, 1).wait()
            if j == 2:
                load_g0(1, 256, 384).wait()
            sb1[0, 0, r:r + h, c:c + w] = piece(j, 0).astype(jnp.bfloat16)
            term_piece(j).start()
            if j:
                send(j - 1)
            if j < 2:
                load_half(2, j).wait()
            total[r:r + h, c:c + w] = piece(j, 2)
            if j == 0:
                load_g(1).start()
                load_a(0, 1).start()
                load_a(0, 3).start()
        send(len(PIECES) - 1)
        load_g(2).start()

    def next_a(k, i):
        @pl.when((k % per == per - 1) & (k + 1 < chunks))
        def _():
            load_a(k // per + 1, i).start()
            load_a(k // per + 1, i + 2).start()

    def reduce_part(k):
        first = k % per == 0
        load_g(k).wait()

        @pl.when(first)
        def _():
            load_a(k // per, 0).wait()
            load_a(k // per, 2).wait()

        @pl.when(k == 2)
        def _():
            for j in range(len(PIECES)):
                term_piece(j).wait_send()

        @pl.when(k > 2)
        def _():
            term(k - 2, 0).wait_send()

        sb1[k % 2, 0] = product(k, 0).astype(jnp.bfloat16)
        term(k, 0).start()
        total[...] = product(k, 2)
        next_a(k, 0)
        term(k, 0).wait_recv()

        @pl.when(k == 2)
        def _():
            for j in range(len(PIECES)):
                half_piece(j).wait_send()

        @pl.when(k > 2)
        def _():
            half(k - 2).wait_send()

        sb2[k % 2] = both(total[...], rv1[k % 2, 0]).astype(jnp.bfloat16)
        half(k).start()

    def owner_part(k):
        @pl.when(k % per == 0)
        def _():
            load_a(k // per, 1).wait()
            load_a(k // per, 3).wait()

        @pl.when(k >= 2)
        def _():
            term(k - 2, 1).wait_send()

        sb1[k % 2, 1] = product(k, 1).astype(jnp.bfloat16)
        term(k, 1).start()
        total[...] = product(k, 3)

        @pl.when(k + 3 < chunks)
        def _():
            load_g(k + 3).start()

        next_a(k, 1)
        term(k, 1).wait_recv()

        @pl.when(k == 0)
        def _():
            for j in range(len(PIECES)):
                half_piece(j).wait_recv()

        @pl.when(k > 0)
        def _():
            half(k).wait_recv()

        out[k, rows(dp)] = both(both(total[...], rv1[k % 2, 1]), rv2[k % RING]).astype(jnp.bfloat16)

        @pl.when(k < inside - 1)
        def _():
            cross(k).start()

        give(k).start()

    load_half(0, 0).start()
    load_g0(0, 0, 256).start()
    load_half(2, 0).start()
    load_half(0, 1).start()
    load_half(2, 1).start()
    load_g0(1, 256, 384).start()
    barrier = pltpu.get_barrier_semaphore()
    for other in (partner, peer):
        pl.semaphore_signal(barrier, inc=1, device_id=(rep, other), device_id_type=MESH)
    pl.semaphore_wait(barrier, 2)
    first_part()

    def step(k, _):
        @pl.when(k + 1 < chunks)
        def _():
            reduce_part(k + 1)

        @pl.when(k == inside)
        def _():
            cross_last().start()

        owner_part(k)

        @pl.when((k >= 2) & (k < inside + 1))
        def _():
            cross(k - 2).wait_recv()
            forward(k - 2).start()

    lax.fori_loop(0, chunks, step, None)
    tail = lb.shape[0]
    la[:quarter] = out[chunks - 2, rows(dp)]
    la[quarter:] = out[chunks - 1, rows(dp, 0, quarter - tail)]
    lb[...] = out[chunks - 1, rows(dp, quarter - tail, tail)]

    for k in range(chunks - 2, chunks):
        for i in range(2):
            term(k, i).wait_send()
        half(k).wait_send()

    for k in range(inside - 1, chunks):
        give(k).wait()

    def drain(k, _):
        cross(k).wait_send()
        give(k).wait()
        forward(k).wait()

    lax.fori_loop(0, inside - 1, drain, None)
    cross_last().wait()


def write(done, out, sem):
    chunks = done.shape[0]
    per = chunks // out.shape[0]

    def copy(k):
        return pltpu.make_async_copy(done.at[k], out.at[k // per, :, pl.ds((k % per) * WIDTH, WIDTH)], sem.at[k])

    for k in range(chunks):
        copy(k).start()
    for k in range(chunks):
        copy(k).wait()


def patch(spots, *refs):
    parts, out, sem = refs[:-3], refs[-2], refs[-1]
    _, dim, wide = out.shape
    per = wide // WIDTH
    dp = lax.axis_index("dp")
    copies = []
    for i, pieces in enumerate(spots):
        start = 0
        for k, row, size in pieces:
            for j, q in enumerate(((dp + 2) % 4, 3 - dp)):
                rows = pl.ds(pl.multiple_of(q * (dim // 4) + row, 128), size)
                copies.append(pltpu.make_async_copy(
                    parts[2 * i + j].at[pl.ds(start, size)],
                    out.at[k // per, rows, pl.ds((k % per) * WIDTH, WIDTH)], sem.at[len(copies)]))
            start += size
    for copy in copies:
        copy.start()
    for copy in copies:
        copy.wait()


def solution(mesh):
    def step(a, g):
        _, mats, tokens, dim = a.shape
        wide = g.shape[3]
        chunks = mats * (wide // WIDTH)
        block = (dim // 4, WIDTH)
        dma = pltpu.SemaphoreType.DMA
        bf16, f32 = jnp.bfloat16, jnp.float32
        pieces = len(PIECES)
        quarter = dim // 4
        done, got, la, lb = pl.pallas_call(
            kernel,
            out_shape=tuple(pltpu.VMEM(shape, bf16) for shape in (
                (chunks, dim, WIDTH), block, (2 * quarter - TAIL, WIDTH), (TAIL, WIDTH))),
            in_specs=[pl.BlockSpec(memory_space=pl.ANY)] * 2,
            out_specs=(pl.BlockSpec(memory_space=pltpu.VMEM),) * 4,
            scratch_shapes=[
                pltpu.VMEM((tokens, dim), bf16),
                pltpu.VMEM((3, tokens, WIDTH), bf16),
                pltpu.VMEM((2, 2, *block), bf16),
                pltpu.VMEM((2, 2, *block), bf16),
                pltpu.VMEM(block, f32),
                pltpu.VMEM((2, *block), bf16),
                pltpu.VMEM((RING, *block), bf16),
                dma((4,)), dma((2, 2)), dma((3,)), dma((2,)),
                dma((2, 2)), dma((chunks, 2)), dma((pieces,)), dma((pieces,)),
                dma((2,)), dma((chunks,)), dma((pieces,)), dma((pieces,)),
                dma((chunks,)), dma((chunks,)),
                dma((chunks,)), dma((chunks,)),
                dma((chunks,)), dma((chunks,)),
            ],
            compiler_params=pltpu.CompilerParams(
                collective_id=0, has_side_effects=True, vmem_limit_bytes=38_000_000),
            name="reduce",
        )(a, g)

        def across(x):
            return lax.ppermute(x, "dp", [(d, (d + 2) % 4) for d in range(4)])

        def beside(x):
            return lax.ppermute(x, "dp", [(d, d ^ 1) for d in range(4)])

        def patched(out, spots, *parts):
            return pl.pallas_call(
                functools.partial(patch, spots),
                out_shape=jax.ShapeDtypeStruct(out.shape, out.dtype),
                in_specs=[pl.BlockSpec(memory_space=pltpu.VMEM)] * len(parts) + [pl.BlockSpec(memory_space=pl.ANY)],
                out_specs=pl.BlockSpec(memory_space=pl.ANY),
                input_output_aliases={len(parts): 0},
                scratch_shapes=[dma((2 * sum(len(s) for s in spots),))],
                compiler_params=pltpu.CompilerParams(vmem_limit_bytes=1_000_000),
            )(*parts, out)

        near_a = across(la)
        near_b = across(lb)
        got_far = beside(got)
        out = pl.pallas_call(
            write,
            out_shape=jax.ShapeDtypeStruct((mats, dim, wide), bf16),
            in_specs=[pl.BlockSpec(memory_space=pltpu.VMEM)],
            out_specs=pl.BlockSpec(memory_space=pl.ANY),
            scratch_shapes=[dma((chunks,))],
            compiler_params=pltpu.CompilerParams(vmem_limit_bytes=1_000_000),
            name="write",
        )(done)
        far_a = beside(near_a)
        far_b = beside(near_b)
        end = chunks - 1
        out = patched(
            out, (((end - 2, 0, quarter),), ((end - 1, 0, quarter), (end, 0, quarter - TAIL))),
            got, got_far, near_a, far_a)
        return patched(out, (((end, quarter - TAIL, TAIL),),), near_b, far_b)

    both = P(("rep", "dp"))
    return jax.shard_map(step, mesh=mesh, in_specs=(both, both), out_specs=P("rep"), check_vma=False)
```

```python
import functools

import jax
import jax.numpy as jnp
from jax import lax
from jax.experimental import pallas as pl
from jax.experimental.pallas import tpu as pltpu
from jax.sharding import PartitionSpec as P


MESH = pl.DeviceIdType.MESH
WIDTH = 640
RING = 4
SPLIT = 192
PIECES = ((0, 0, 128, 0, 256), (0, 128, 128, 0, 256), (0, 0, 128, 256, 384), (0, 128, 128, 256, 384), (1, 0, 256, 0, 256), (1, 0, 256, 256, 384))
LAST = 2
TAIL = 128


def kernel(
    a, g, out, got, la, lb, abuf, gbuf, sb1, rv1, total, sb2, rv2,
    asem, hsem, gsem, g0sem, s1, r1, p1, q1, s2, r2, p2, q2, s3, r3, s4, r4, s5, r5, s6, r6, turn,
):
    _, mats, _, dim = a.shape
    quarter = dim // 4
    per = g.shape[3] // WIDTH
    chunks = mats * per
    inside = chunks - LAST
    rep, dp = lax.axis_index("rep"), lax.axis_index("dp")
    partner = 2 * (dp // 2) + 1 - dp % 2
    peer = (dp + 2) % 4
    order = (3 - dp, partner, peer, dp)

    def rows(q, start=0, size=quarter):
        return pl.ds(pl.multiple_of(q * quarter + start, 128), size)

    def columns(k):
        return pl.ds(pl.multiple_of((k % per) * WIDTH, 128), WIDTH)

    def place(k, q):
        return out.at[k, rows(q)]

    def load_a(n, i):
        return pltpu.make_async_copy(
            a.at[0, n, :, rows(order[i])], abuf.at[:, rows(order[i])], asem.at[i])

    def load_half(i, h):
        part = rows(order[i], h * 128, 128)
        return pltpu.make_async_copy(a.at[0, 0, :, part], abuf.at[:, part], hsem.at[i // 2, h])

    def load_g(k):
        return pltpu.make_async_copy(g.at[0, k // per, :, columns(k)], gbuf.at[k % 3], gsem.at[k % 3])

    def load_g0(j, start, size):
        part = pl.ds(start, size)
        return pltpu.make_async_copy(g.at[0, 0, :, part], gbuf.at[0, :, part], g0sem.at[j])

    def remote(src, dst, send, recv, to):
        return pltpu.make_async_remote_copy(
            src_ref=src, dst_ref=dst, send_sem=send, recv_sem=recv,
            device_id=(rep, to), device_id_type=MESH)

    def term(k, i):
        return remote(sb1.at[k % 2, i], rv1.at[k % 2, i], s1.at[k % 2, i], r1.at[k, i], partner)

    def term_piece(j):
        k, r, h, c, w = PIECES[j]
        part = (pl.ds(r, h), pl.ds(c, w))
        return remote(sb1.at[k, 0, *part], rv1.at[k, 0, *part], p1.at[j], q1.at[j], partner)

    def half(k):
        return remote(sb2.at[k % 2], rv2.at[k % RING], s2.at[k % 2], r2.at[k], peer)

    def half_piece(j):
        k, r, h, c, w = PIECES[j]
        part = (pl.ds(r, h), pl.ds(c, w))
        return remote(sb2.at[k, *part], rv2.at[k, *part], p2.at[j], q2.at[j], peer)

    def give(k):
        return remote(place(k, dp), place(k, dp), s3.at[k], r3.at[k], partner)

    def cross(k):
        return remote(place(k, dp), place(k, dp), s4.at[k], r4.at[k], peer)

    def cross_last(j):
        start, size = ((0, SPLIT), (SPLIT, quarter - SPLIT))[j]
        return remote(out.at[inside - 1, pl.ds(pl.multiple_of(dp * quarter + start, 16), size)],
                      got.at[pl.ds(start, size)], s6.at[j], r6.at[j], peer)

    def forward(k):
        return remote(place(k, peer), place(k, peer), s5.at[k], r5.at[k], partner)

    def dot(left, right):
        return lax.dot_general(left, right, (((0,), (0,)), ((), ())), preferred_element_type=jnp.float32)

    def product(k, i):
        return dot(abuf[:, rows(order[i])], gbuf[k % 3])

    def both(here, there):
        return here + there.astype(jnp.float32)

    def first_part():
        def piece(j, i):
            k, r, h, c, w = PIECES[j]
            return dot(abuf[:, rows(order[i], r, h)], gbuf[k, :, c:c + w])

        def send(j):
            k, r, h, c, w = PIECES[j]
            term_piece(j).wait_recv()
            sb2[k, r:r + h, c:c + w] = both(total[r:r + h, c:c + w], rv1[k, 0, r:r + h, c:c + w]).astype(jnp.bfloat16)
            half_piece(j).start()

        waited = set()

        def need(name, load, *args):
            if name not in waited:
                waited.add(name)
                load(*args).wait()

        for j, (k, r, h, c, w) in enumerate(PIECES):
            halves = [x for x in range(2) if k == 0 and r < (x + 1) * 128 and r + h > x * 128]
            for x in halves:
                need((0, x), load_half, 0, x)
            if k == 0 and c < 256:
                need("g", load_g0, 0, 0, 256)
            if k == 0 and c + w > 256:
                need("h", load_g0, 1, 256, 384)
            if k == 1:
                need("k", load_g, 1)
            sb1[k, 0, r:r + h, c:c + w] = piece(j, 0).astype(jnp.bfloat16)
            if j == 0:
                pl.semaphore_wait(pltpu.get_barrier_semaphore(), 2)
            term_piece(j).start()
            if j:
                send(j - 1)
            for x in halves:
                need((2, x), load_half, 2, x)
            total[r:r + h, c:c + w] = piece(j, 2)
            if j == 0:
                load_g(1).start()
                load_a(0, 1).start()
                load_a(0, 3).start()
        send(len(PIECES) - 1)
        load_g(2).start()

    def pieces_of(k, act):
        for j in range(len(PIECES)):
            if PIECES[j][0] == k:
                act(j)

    def next_a(k, i):
        @pl.when((k % per == per - 1) & (k + 1 < chunks))
        def _():
            load_a(k // per + 1, i).start()
            load_a(k // per + 1, i + 2).start()

    def reduce_part(k):
        first = k % per == 0
        load_g(k).wait()

        @pl.when(first)
        def _():
            load_a(k // per, 0).wait()
            load_a(k // per, 2).wait()

        for early in range(2):
            @pl.when(k == early + 2)
            def _():
                pieces_of(early, lambda j: term_piece(j).wait_send())
                pieces_of(early, lambda j: half_piece(j).wait_send())

        @pl.when(k > 3)
        def _():
            term(k - 2, 0).wait_send()

        sb1[k % 2, 0] = product(k, 0).astype(jnp.bfloat16)
        term(k, 0).start()
        total[...] = product(k, 2)
        next_a(k, 0)
        term(k, 0).wait_recv()

        @pl.when(k > 3)
        def _():
            half(k - 2).wait_send()

        sb2[k % 2] = both(total[...], rv1[k % 2, 0]).astype(jnp.bfloat16)
        half(k).start()

    def owner_part(k):
        @pl.when(k % per == 0)
        def _():
            load_a(k // per, 1).wait()
            load_a(k // per, 3).wait()

        @pl.when(k >= 2)
        def _():
            term(k - 2, 1).wait_send()

        sb1[k % 2, 1] = product(k, 1).astype(jnp.bfloat16)
        term(k, 1).start()
        total[...] = product(k, 3)

        @pl.when(k + 3 < chunks)
        def _():
            load_g(k + 3).start()

        next_a(k, 1)
        term(k, 1).wait_recv()

        for early in range(2):
            @pl.when(k == early)
            def _():
                pieces_of(early, lambda j: half_piece(j).wait_recv())

        @pl.when(k > 1)
        def _():
            half(k).wait_recv()

        out[k, rows(dp)] = both(both(total[...], rv1[k % 2, 1]), rv2[k % RING]).astype(jnp.bfloat16)

        @pl.when(k < inside - 1)
        def _():
            cross(k).start()

        give(k).start()

    load_half(0, 0).start()
    load_g0(0, 0, 256).start()
    load_half(2, 0).start()
    load_half(0, 1).start()
    load_half(2, 1).start()
    load_g0(1, 256, 384).start()
    barrier = pltpu.get_barrier_semaphore()
    for other in (partner, peer):
        pl.semaphore_signal(barrier, inc=1, device_id=(rep, other), device_id_type=MESH)
    first_part()

    def step(k, _):
        @pl.when((k > 0) & (k + 1 < chunks))
        def _():
            reduce_part(k + 1)

        @pl.when((k == inside) & (dp % 2 == 0))
        def _():
            cross_last(0).start()
            cross_last(1).start()

        owner_part(k)

        @pl.when((k >= 2) & (k < inside + 1))
        def _():
            cross(k - 2).wait_recv()
            forward(k - 2).start()

    lax.fori_loop(0, chunks, step, None)

    @pl.when(dp % 2 == 0)
    def _():
        cross_last(0).wait_send()
        pl.semaphore_signal(turn, inc=1, device_id=(rep, partner), device_id_type=MESH)

    @pl.when(dp % 2 == 1)
    def _():
        pl.semaphore_wait(turn, 1)
        cross_last(0).start()
        cross_last(1).start()
        cross_last(0).wait_send()

    tail = lb.shape[0]
    la[:quarter] = out[chunks - 2, rows(dp)]
    la[quarter:] = out[chunks - 1, rows(dp, 0, quarter - tail)]
    lb[...] = out[chunks - 1, rows(dp, quarter - tail, tail)]

    for k in range(chunks - 2, chunks):
        for i in range(2):
            term(k, i).wait_send()
        half(k).wait_send()

    for k in range(inside - 1, chunks):
        give(k).wait()

    def drain(k, _):
        cross(k).wait_send()
        give(k).wait()
        forward(k).wait()

    lax.fori_loop(0, inside - 1, drain, None)
    cross_last(0).wait_recv()
    cross_last(1).wait()


def write(done, out, sem):
    chunks = done.shape[0]
    per = chunks // out.shape[0]

    def copy(k):
        return pltpu.make_async_copy(done.at[k], out.at[k // per, :, pl.ds((k % per) * WIDTH, WIDTH)], sem.at[k])

    for k in range(chunks):
        copy(k).start()
    for k in range(chunks):
        copy(k).wait()


def patch(spots, *refs):
    parts, out, sem = refs[:-3], refs[-2], refs[-1]
    _, dim, wide = out.shape
    per = wide // WIDTH
    dp = lax.axis_index("dp")
    copies = []
    for i, pieces in enumerate(spots):
        start = 0
        for k, row, size in pieces:
            for j, q in enumerate(((dp + 2) % 4, 3 - dp)):
                rows = pl.ds(pl.multiple_of(q * (dim // 4) + row, 128), size)
                copies.append(pltpu.make_async_copy(
                    parts[2 * i + j].at[pl.ds(start, size)],
                    out.at[k // per, rows, pl.ds((k % per) * WIDTH, WIDTH)], sem.at[len(copies)]))
            start += size
    for copy in copies:
        copy.start()
    for copy in copies:
        copy.wait()


def solution(mesh):
    def step(a, g):
        _, mats, tokens, dim = a.shape
        wide = g.shape[3]
        chunks = mats * (wide // WIDTH)
        block = (dim // 4, WIDTH)
        dma = pltpu.SemaphoreType.DMA
        bf16, f32 = jnp.bfloat16, jnp.float32
        pieces = len(PIECES)
        quarter = dim // 4
        done, got, la, lb = pl.pallas_call(
            kernel,
            out_shape=tuple(pltpu.VMEM(shape, bf16) for shape in (
                (chunks, dim, WIDTH), block, (2 * quarter - TAIL, WIDTH), (TAIL, WIDTH))),
            in_specs=[pl.BlockSpec(memory_space=pl.ANY)] * 2,
            out_specs=(pl.BlockSpec(memory_space=pltpu.VMEM),) * 4,
            scratch_shapes=[
                pltpu.VMEM((tokens, dim), bf16),
                pltpu.VMEM((3, tokens, WIDTH), bf16),
                pltpu.VMEM((2, 2, *block), bf16),
                pltpu.VMEM((2, 2, *block), bf16),
                pltpu.VMEM(block, f32),
                pltpu.VMEM((2, *block), bf16),
                pltpu.VMEM((RING, *block), bf16),
                dma((4,)), dma((2, 2)), dma((3,)), dma((2,)),
                dma((2, 2)), dma((chunks, 2)), dma((pieces,)), dma((pieces,)),
                dma((2,)), dma((chunks,)), dma((pieces,)), dma((pieces,)),
                dma((chunks,)), dma((chunks,)),
                dma((chunks,)), dma((chunks,)),
                dma((chunks,)), dma((chunks,)), dma((2,)), dma((2,)), pltpu.SemaphoreType.REGULAR,
            ],
            compiler_params=pltpu.CompilerParams(
                collective_id=0, has_side_effects=True, vmem_limit_bytes=38_000_000),
            name="reduce",
        )(a, g)

        def across(x):
            return lax.ppermute(x, "dp", [(d, (d + 2) % 4) for d in range(4)])

        def beside(x):
            return lax.ppermute(x, "dp", [(d, d ^ 1) for d in range(4)])

        def patched(out, spots, *parts):
            return pl.pallas_call(
                functools.partial(patch, spots),
                out_shape=jax.ShapeDtypeStruct(out.shape, out.dtype),
                in_specs=[pl.BlockSpec(memory_space=pltpu.VMEM)] * len(parts) + [pl.BlockSpec(memory_space=pl.ANY)],
                out_specs=pl.BlockSpec(memory_space=pl.ANY),
                input_output_aliases={len(parts): 0},
                scratch_shapes=[dma((2 * sum(len(s) for s in spots),))],
                compiler_params=pltpu.CompilerParams(vmem_limit_bytes=1_000_000),
            )(*parts, out)

        near_a = across(la)
        near_b = across(lb)
        got_far = beside(got)
        out = pl.pallas_call(
            write,
            out_shape=jax.ShapeDtypeStruct((mats, dim, wide), bf16),
            in_specs=[pl.BlockSpec(memory_space=pltpu.VMEM)],
            out_specs=pl.BlockSpec(memory_space=pl.ANY),
            scratch_shapes=[dma((chunks,))],
            compiler_params=pltpu.CompilerParams(vmem_limit_bytes=1_000_000),
            name="write",
        )(done)
        far_a = beside(near_a)
        far_b = beside(near_b)
        end = chunks - 1
        out = patched(
            out, (((end - 2, 0, quarter),), ((end - 1, 0, quarter), (end, 0, quarter - TAIL))),
            got, got_far, near_a, far_a)
        return patched(out, (((end, quarter - TAIL, TAIL),),), near_b, far_b)

    both = P(("rep", "dp"))
    return jax.shard_map(step, mesh=mesh, in_specs=(both, both), out_specs=P("rep"), check_vma=False)
```

```python
import functools

import jax
import jax.numpy as jnp
from jax import lax
from jax.experimental import pallas as pl
from jax.experimental.pallas import tpu as pltpu
from jax.sharding import PartitionSpec as P


MESH = pl.DeviceIdType.MESH
WIDTH = 640
RING = 4
SPLIT = 192
PIECES = ((0, 0, 128, 0, 256), (0, 128, 128, 0, 256), (0, 0, 128, 256, 384), (0, 128, 128, 256, 384), (1, 0, 256, 0, 256), (1, 0, 256, 256, 384))
LAST = 2
TAIL = 128


def kernel(
    a, g, out, got, la, lb, abuf, gbuf, sb1, rv1, total, sb2, rv2,
    asem, hsem, gsem, g0sem, s1, r1, q1, s2, r2, s3, r3, s4, r4, s5, r5, s6, r6, turn,
):
    _, mats, _, dim = a.shape
    quarter = dim // 4
    per = g.shape[3] // WIDTH
    chunks = mats * per
    inside = chunks - LAST
    rep, dp = lax.axis_index("rep"), lax.axis_index("dp")
    partner = 2 * (dp // 2) + 1 - dp % 2
    peer = (dp + 2) % 4
    order = (3 - dp, partner, peer, dp)

    def rows(q, start=0, size=quarter):
        return pl.ds(pl.multiple_of(q * quarter + start, 128), size)

    def columns(k):
        return pl.ds(pl.multiple_of((k % per) * WIDTH, 128), WIDTH)

    def place(k, q):
        return out.at[k, rows(q)]

    def load_a(n, i):
        return pltpu.make_async_copy(
            a.at[0, n, :, rows(order[i])], abuf.at[:, rows(order[i])], asem.at[i])

    def load_half(i, h):
        part = rows(order[i], h * 128, 128)
        return pltpu.make_async_copy(a.at[0, 0, :, part], abuf.at[:, part], hsem.at[i // 2, h])

    def load_g(k):
        return pltpu.make_async_copy(g.at[0, k // per, :, columns(k)], gbuf.at[k % 3], gsem.at[k % 3])

    def load_g0(j, start, size):
        part = pl.ds(start, size)
        return pltpu.make_async_copy(g.at[0, 0, :, part], gbuf.at[0, :, part], g0sem.at[j])

    def remote(src, dst, send, recv, to):
        return pltpu.make_async_remote_copy(
            src_ref=src, dst_ref=dst, send_sem=send, recv_sem=recv,
            device_id=(rep, to), device_id_type=MESH)

    def term(k, i):
        return remote(sb1.at[k % 2, i], rv1.at[k % 2, i], s1.at[k % 2, i], r1.at[k % 2, i], partner)

    def term_piece(j):
        k, r, h, c, w = PIECES[j]
        part = (pl.ds(r, h), pl.ds(c, w))
        return remote(sb1.at[k, 0, *part], rv1.at[k, 0, *part], s1.at[k, 0], q1.at[j % 4], partner)

    def half(k):
        return remote(sb2.at[k % 2], rv2.at[k % RING], s2.at[k % 2], r2.at[k % RING], peer)

    def half_piece(j):
        k, r, h, c, w = PIECES[j]
        part = (pl.ds(r, h), pl.ds(c, w))
        return remote(sb2.at[k, *part], rv2.at[k, *part], s2.at[k], r2.at[k], peer)

    def give(k):
        return remote(place(k, dp), place(k, dp), s3.at[k % RING], r3.at[k % RING], partner)

    def cross(k):
        return remote(place(k, dp), place(k, dp), s4.at[k % RING], r4.at[k % RING], peer)

    def cross_last(j):
        start, size = ((0, SPLIT), (SPLIT, quarter - SPLIT))[j]
        return remote(out.at[inside - 1, pl.ds(pl.multiple_of(dp * quarter + start, 16), size)],
                      got.at[pl.ds(start, size)], s6.at[j], r6.at[j], peer)

    def forward(k):
        return remote(place(k, peer), place(k, peer), s5.at[k % RING], r5.at[k % RING], partner)

    def dot(left, right):
        return lax.dot_general(left, right, (((0,), (0,)), ((), ())), preferred_element_type=jnp.float32)

    def product(k, i):
        return dot(abuf[:, rows(order[i])], gbuf[k % 3])

    def both(here, there):
        return here + there.astype(jnp.float32)

    def first_part():
        def piece(j, i):
            k, r, h, c, w = PIECES[j]
            return dot(abuf[:, rows(order[i], r, h)], gbuf[k, :, c:c + w])

        def send(j):
            k, r, h, c, w = PIECES[j]
            term_piece(j).wait_recv()
            sb2[k, r:r + h, c:c + w] = both(total[r:r + h, c:c + w], rv1[k, 0, r:r + h, c:c + w]).astype(jnp.bfloat16)
            half_piece(j).start()

        waited = set()

        def need(name, load, *args):
            if name not in waited:
                waited.add(name)
                load(*args).wait()

        for j, (k, r, h, c, w) in enumerate(PIECES):
            halves = [x for x in range(2) if k == 0 and r < (x + 1) * 128 and r + h > x * 128]
            for x in halves:
                need((0, x), load_half, 0, x)
            if k == 0 and c < 256:
                need("g", load_g0, 0, 0, 256)
            if k == 0 and c + w > 256:
                need("h", load_g0, 1, 256, 384)
            if k == 1:
                need("k", load_g, 1)
            sb1[k, 0, r:r + h, c:c + w] = piece(j, 0).astype(jnp.bfloat16)
            if j == 0:
                pl.semaphore_wait(pltpu.get_barrier_semaphore(), 2)
            term_piece(j).start()
            if j:
                send(j - 1)
            for x in halves:
                need((2, x), load_half, 2, x)
            total[r:r + h, c:c + w] = piece(j, 2)
            if j == 0:
                load_g(1).start()
                load_a(0, 1).start()
                load_a(0, 3).start()
        send(len(PIECES) - 1)
        load_g(2).start()

    def next_a(k, i):
        @pl.when((k % per == per - 1) & (k + 1 < chunks))
        def _():
            load_a(k // per + 1, i).start()
            load_a(k // per + 1, i + 2).start()

    def reduce_part(k):
        first = k % per == 0
        load_g(k).wait()

        @pl.when(first)
        def _():
            load_a(k // per, 0).wait()
            load_a(k // per, 2).wait()

        term(k - 2, 0).wait_send()

        sb1[k % 2, 0] = product(k, 0).astype(jnp.bfloat16)
        term(k, 0).start()
        total[...] = product(k, 2)
        next_a(k, 0)
        term(k, 0).wait_recv()

        half(k - 2).wait_send()

        sb2[k % 2] = both(total[...], rv1[k % 2, 0]).astype(jnp.bfloat16)
        half(k).start()

    def owner_part(k):
        @pl.when(k % per == 0)
        def _():
            load_a(k // per, 1).wait()
            load_a(k // per, 3).wait()

        @pl.when(k >= 2)
        def _():
            term(k - 2, 1).wait_send()

        sb1[k % 2, 1] = product(k, 1).astype(jnp.bfloat16)
        term(k, 1).start()
        total[...] = product(k, 3)

        @pl.when(k + 3 < chunks)
        def _():
            load_g(k + 3).start()

        next_a(k, 1)
        term(k, 1).wait_recv()

        half(k).wait_recv()

        out[k, rows(dp)] = both(both(total[...], rv1[k % 2, 1]), rv2[k % RING]).astype(jnp.bfloat16)

        @pl.when((k >= RING) & (k < inside - 1))
        def _():
            cross(k - RING).wait_send()

        @pl.when(k < inside - 1)
        def _():
            cross(k).start()

        @pl.when(k >= RING)
        def _():
            give(k - RING).wait_send()

        give(k).start()

    load_half(0, 0).start()
    load_g0(0, 0, 256).start()
    load_half(2, 0).start()
    load_half(0, 1).start()
    load_half(2, 1).start()
    load_g0(1, 256, 384).start()
    barrier = pltpu.get_barrier_semaphore()
    for other in (partner, peer):
        pl.semaphore_signal(barrier, inc=1, device_id=(rep, other), device_id_type=MESH)
    first_part()

    def step(k, _):
        @pl.when((k > 0) & (k + 1 < chunks))
        def _():
            reduce_part(k + 1)

        @pl.when((k == inside) & (dp % 2 == 0))
        def _():
            cross_last(0).start()
            cross_last(1).start()

        owner_part(k)

        @pl.when((k >= 2) & (k < inside + 1))
        def _():
            cross(k - 2).wait_recv()

            @pl.when(k >= RING + 2)
            def _():
                forward(k - RING - 2).wait_send()

            forward(k - 2).start()

        @pl.when(k >= 2)
        def _():
            give(k - 2).wait_recv()

        @pl.when(k >= 4)
        def _():
            forward(k - 4).wait_recv()

    lax.fori_loop(0, chunks, step, None)

    @pl.when(dp % 2 == 0)
    def _():
        cross_last(0).wait_send()
        pl.semaphore_signal(turn, inc=1, device_id=(rep, partner), device_id_type=MESH)

    @pl.when(dp % 2 == 1)
    def _():
        pl.semaphore_wait(turn, 1)
        cross_last(0).start()
        cross_last(1).start()
        cross_last(0).wait_send()

    tail = lb.shape[0]
    la[:quarter] = out[chunks - 2, rows(dp)]
    la[quarter:] = out[chunks - 1, rows(dp, 0, quarter - tail)]
    lb[...] = out[chunks - 1, rows(dp, quarter - tail, tail)]

    for k in range(chunks - 2, chunks):
        for i in range(2):
            term(k, i).wait_send()
        half(k).wait_send()

    for k in range(chunks - RING, chunks):
        give(k).wait_send()
    for k in range(chunks - 2, chunks):
        give(k).wait_recv()
    for k in range(inside - 1 - RING, inside - 1):
        cross(k).wait_send()
        forward(k).wait_send()
    for k in range(chunks - 4, inside - 1):
        forward(k).wait_recv()
    cross_last(0).wait_recv()
    cross_last(1).wait()


def write(done, out, sem):
    chunks = done.shape[0]
    per = chunks // out.shape[0]

    def copy(k):
        return pltpu.make_async_copy(done.at[k], out.at[k // per, :, pl.ds((k % per) * WIDTH, WIDTH)], sem.at[k])

    for k in range(chunks):
        copy(k).start()
    for k in range(chunks):
        copy(k).wait()


def patch(spots, *refs):
    parts, out, sem = refs[:-3], refs[-2], refs[-1]
    _, dim, wide = out.shape
    per = wide // WIDTH
    dp = lax.axis_index("dp")
    copies = []
    for i, pieces in enumerate(spots):
        start = 0
        for k, row, size in pieces:
            for j, q in enumerate(((dp + 2) % 4, 3 - dp)):
                rows = pl.ds(pl.multiple_of(q * (dim // 4) + row, 128), size)
                copies.append(pltpu.make_async_copy(
                    parts[2 * i + j].at[pl.ds(start, size)],
                    out.at[k // per, rows, pl.ds((k % per) * WIDTH, WIDTH)], sem.at[len(copies)]))
            start += size
    for copy in copies:
        copy.start()
    for copy in copies:
        copy.wait()


def solution(mesh):
    def step(a, g):
        _, mats, tokens, dim = a.shape
        wide = g.shape[3]
        chunks = mats * (wide // WIDTH)
        block = (dim // 4, WIDTH)
        dma = pltpu.SemaphoreType.DMA
        bf16, f32 = jnp.bfloat16, jnp.float32
        quarter = dim // 4
        done, got, la, lb = pl.pallas_call(
            kernel,
            out_shape=tuple(pltpu.VMEM(shape, bf16) for shape in (
                (chunks, dim, WIDTH), block, (2 * quarter - TAIL, WIDTH), (TAIL, WIDTH))),
            in_specs=[pl.BlockSpec(memory_space=pl.ANY)] * 2,
            out_specs=(pl.BlockSpec(memory_space=pltpu.VMEM),) * 4,
            scratch_shapes=[
                pltpu.VMEM((tokens, dim), bf16),
                pltpu.VMEM((3, tokens, WIDTH), bf16),
                pltpu.VMEM((2, 2, *block), bf16),
                pltpu.VMEM((2, 2, *block), bf16),
                pltpu.VMEM(block, f32),
                pltpu.VMEM((2, *block), bf16),
                pltpu.VMEM((RING, *block), bf16),
                dma((4,)), dma((2, 2)), dma((3,)), dma((2,)),
                dma((2, 2)), dma((2, 2)), dma((4,)),
                dma((2,)), dma((RING,)),
                dma((RING,)), dma((RING,)),
                dma((RING,)), dma((RING,)),
                dma((RING,)), dma((RING,)), dma((2,)), dma((2,)), pltpu.SemaphoreType.REGULAR,
            ],
            compiler_params=pltpu.CompilerParams(
                collective_id=0, has_side_effects=True, vmem_limit_bytes=38_000_000),
            name="reduce",
        )(a, g)

        def across(x):
            return lax.ppermute(x, "dp", [(d, (d + 2) % 4) for d in range(4)])

        def beside(x):
            return lax.ppermute(x, "dp", [(d, d ^ 1) for d in range(4)])

        def patched(out, spots, *parts):
            return pl.pallas_call(
                functools.partial(patch, spots),
                out_shape=jax.ShapeDtypeStruct(out.shape, out.dtype),
                in_specs=[pl.BlockSpec(memory_space=pltpu.VMEM)] * len(parts) + [pl.BlockSpec(memory_space=pl.ANY)],
                out_specs=pl.BlockSpec(memory_space=pl.ANY),
                input_output_aliases={len(parts): 0},
                scratch_shapes=[dma((2 * sum(len(s) for s in spots),))],
                compiler_params=pltpu.CompilerParams(vmem_limit_bytes=1_000_000),
            )(*parts, out)

        near_a = across(la)
        near_b = across(lb)
        got_far = beside(got)
        out = pl.pallas_call(
            write,
            out_shape=jax.ShapeDtypeStruct((mats, dim, wide), bf16),
            in_specs=[pl.BlockSpec(memory_space=pltpu.VMEM)],
            out_specs=pl.BlockSpec(memory_space=pl.ANY),
            scratch_shapes=[dma((chunks,))],
            compiler_params=pltpu.CompilerParams(vmem_limit_bytes=1_000_000),
            name="write",
        )(done)
        far_a = beside(near_a)
        far_b = beside(near_b)
        end = chunks - 1
        out = patched(
            out, (((end - 2, 0, quarter),), ((end - 1, 0, quarter), (end, 0, quarter - TAIL))),
            got, got_far, near_a, far_a)
        return patched(out, (((end, quarter - TAIL, TAIL),),), near_b, far_b)

    both = P(("rep", "dp"))
    return jax.shard_map(step, mesh=mesh, in_specs=(both, both), out_specs=P("rep"), check_vma=False)
```

```python
import functools

import jax
import jax.numpy as jnp
from jax import lax
from jax.experimental import pallas as pl
from jax.experimental.pallas import tpu as pltpu
from jax.sharding import PartitionSpec as P


MESH = pl.DeviceIdType.MESH
WIDTH = 640
RING = 4
SPLIT = 192
PIECES = ((0, 0, 128, 0, 256), (0, 128, 128, 0, 256), (0, 0, 128, 256, 384), (0, 128, 128, 256, 384), (1, 0, 128, 0, 640), (1, 128, 128, 0, 640))
LAST = 2
TAIL = 128


def kernel(
    a, g, out, got, la, lb, abuf, gbuf, sb1, rv1, total, sb2, rv2,
    asem, hsem, gsem, g0sem, ksem, s1, r1, q1, s2, r2, s3, r3, s4, r4, s5, r5, s6, r6, turn,
):
    _, mats, tokens, dim = a.shape
    quarter = dim // 4
    per = g.shape[3] // WIDTH
    chunks = mats * per
    inside = chunks - LAST
    rep, dp = lax.axis_index("rep"), lax.axis_index("dp")
    partner = 2 * (dp // 2) + 1 - dp % 2
    peer = (dp + 2) % 4
    order = (3 - dp, partner, peer, dp)

    def rows(q, start=0, size=quarter):
        return pl.ds(pl.multiple_of(q * quarter + start, 128), size)

    def columns(k):
        return pl.ds(pl.multiple_of((k % per) * WIDTH, 128), WIDTH)

    def place(k, q):
        return out.at[k, rows(q)]

    def load_a(n, i):
        return pltpu.make_async_copy(
            a.at[0, n, :, rows(order[i])], abuf.at[:, rows(order[i])], asem.at[i])

    def load_half(i, h):
        part = rows(order[i], h * 128, 128)
        return pltpu.make_async_copy(a.at[0, 0, :, part], abuf.at[:, part], hsem.at[i // 2, h])

    def load_first_a(j):
        deep, part = pl.ds(j * (tokens // 2), tokens // 2), rows(order[0], 0, 128)
        return pltpu.make_async_copy(a.at[0, 0, deep, part], abuf.at[deep, part], ksem.at[0, j])

    def load_first_g(j):
        deep, part = pl.ds(j * (tokens // 2), tokens // 2), pl.ds(0, 256)
        return pltpu.make_async_copy(g.at[0, 0, deep, part], gbuf.at[0, deep, part], ksem.at[1, j])

    def load_g(k):
        return pltpu.make_async_copy(g.at[0, k // per, :, columns(k)], gbuf.at[k % 3], gsem.at[k % 3])

    def load_g0(j, start, size):
        part = pl.ds(start, size)
        return pltpu.make_async_copy(g.at[0, 0, :, part], gbuf.at[0, :, part], g0sem.at[j])

    def remote(src, dst, send, recv, to):
        return pltpu.make_async_remote_copy(
            src_ref=src, dst_ref=dst, send_sem=send, recv_sem=recv,
            device_id=(rep, to), device_id_type=MESH)

    def term(k, i):
        return remote(sb1.at[k % 2, i], rv1.at[k % 2, i], s1.at[k % 2, i], r1.at[k % 2, i], partner)

    def term_piece(j):
        k, r, h, c, w = PIECES[j]
        part = (pl.ds(r, h), pl.ds(c, w))
        return remote(sb1.at[k, 0, *part], rv1.at[k, 0, *part], s1.at[k, 0], q1.at[j % 4], partner)

    def half(k):
        return remote(sb2.at[k % 2], rv2.at[k % RING], s2.at[k % 2], r2.at[k % RING], peer)

    def half_piece(j):
        k, r, h, c, w = PIECES[j]
        part = (pl.ds(r, h), pl.ds(c, w))
        return remote(sb2.at[k, *part], rv2.at[k, *part], s2.at[k], r2.at[k], peer)

    def give(k):
        return remote(place(k, dp), place(k, dp), s3.at[k % RING], r3.at[k % RING], partner)

    def cross(k):
        return remote(place(k, dp), place(k, dp), s4.at[k % RING], r4.at[k % RING], peer)

    def cross_last(j):
        start, size = ((0, SPLIT), (SPLIT, quarter - SPLIT))[j]
        return remote(out.at[inside - 1, pl.ds(pl.multiple_of(dp * quarter + start, 16), size)],
                      got.at[pl.ds(start, size)], s6.at[j], r6.at[j], peer)

    def forward(k):
        return remote(place(k, peer), place(k, peer), s5.at[k % RING], r5.at[k % RING], partner)

    def dot(left, right):
        return lax.dot_general(left, right, (((0,), (0,)), ((), ())), preferred_element_type=jnp.float32)

    def product(k, i):
        return dot(abuf[:, rows(order[i])], gbuf[k % 3])

    def both(here, there):
        return here + there.astype(jnp.float32)

    def first_part():
        def piece(j, i):
            k, r, h, c, w = PIECES[j]
            return dot(abuf[:, rows(order[i], r, h)], gbuf[k, :, c:c + w])

        def send(j):
            k, r, h, c, w = PIECES[j]
            term_piece(j).wait_recv()
            sb2[k, r:r + h, c:c + w] = both(total[r:r + h, c:c + w], rv1[k, 0, r:r + h, c:c + w]).astype(jnp.bfloat16)
            half_piece(j).start()

        waited = set()

        def need(name, load, *args):
            if name not in waited:
                waited.add(name)
                load(*args).wait()

        for j, (k, r, h, c, w) in enumerate(PIECES):
            halves = [x for x in range(2) if k == 0 and r < (x + 1) * 128 and r + h > x * 128]
            if j == 0:
                for d in range(2):
                    load_first_a(d).wait()
                    load_first_g(d).wait()
                    deep = slice(d * (tokens // 2), (d + 1) * (tokens // 2))
                    part = dot(abuf[deep, rows(order[0], 0, 128)], gbuf[0, deep, :256])
                    total[:128, :256] = part if d == 0 else total[:128, :256] + part
            elif k == 0:
                for x in halves:
                    if x:
                        need((0, x), load_half, 0, x)
            if k == 0 and c + w > 256:
                need("h", load_g0, 1, 256, 384)
            if k == 1:
                need("k", load_g, 1)
            own = total[:128, :256] if j == 0 else piece(j, 0)
            sb1[k, 0, r:r + h, c:c + w] = own.astype(jnp.bfloat16)
            if j == 0:
                pl.semaphore_wait(pltpu.get_barrier_semaphore(), 2)
            term_piece(j).start()
            if j:
                send(j - 1)
            for x in halves:
                need((2, x), load_half, 2, x)
            total[r:r + h, c:c + w] = piece(j, 2)
            if j == 0:
                load_g(1).start()
                load_a(0, 1).start()
                load_a(0, 3).start()
        send(len(PIECES) - 1)
        load_g(2).start()

    def next_a(k, i):
        @pl.when((k % per == per - 1) & (k + 1 < chunks))
        def _():
            load_a(k // per + 1, i).start()
            load_a(k // per + 1, i + 2).start()

    def reduce_part(k):
        first = k % per == 0
        load_g(k).wait()

        @pl.when(first)
        def _():
            load_a(k // per, 0).wait()
            load_a(k // per, 2).wait()

        term(k - 2, 0).wait_send()

        sb1[k % 2, 0] = product(k, 0).astype(jnp.bfloat16)
        term(k, 0).start()
        total[...] = product(k, 2)
        next_a(k, 0)
        term(k, 0).wait_recv()

        half(k - 2).wait_send()

        sb2[k % 2] = both(total[...], rv1[k % 2, 0]).astype(jnp.bfloat16)
        half(k).start()

    def owner_part(k):
        @pl.when(k % per == 0)
        def _():
            load_a(k // per, 1).wait()
            load_a(k // per, 3).wait()

        @pl.when(k >= 2)
        def _():
            term(k - 2, 1).wait_send()

        sb1[k % 2, 1] = product(k, 1).astype(jnp.bfloat16)
        term(k, 1).start()
        total[...] = product(k, 3)

        @pl.when(k + 3 < chunks)
        def _():
            load_g(k + 3).start()

        next_a(k, 1)
        term(k, 1).wait_recv()

        half(k).wait_recv()

        out[k, rows(dp)] = both(both(total[...], rv1[k % 2, 1]), rv2[k % RING]).astype(jnp.bfloat16)

        @pl.when((k >= RING) & (k < inside - 1))
        def _():
            cross(k - RING).wait_send()

        @pl.when(k < inside - 1)
        def _():
            cross(k).start()

        @pl.when(k >= RING)
        def _():
            give(k - RING).wait_send()

        give(k).start()

    for j in range(2):
        load_first_a(j).start()
        load_first_g(j).start()
    load_half(2, 0).start()
    load_half(0, 1).start()
    load_half(2, 1).start()
    load_g0(1, 256, 384).start()
    barrier = pltpu.get_barrier_semaphore()
    for other in (partner, peer):
        pl.semaphore_signal(barrier, inc=1, device_id=(rep, other), device_id_type=MESH)
    first_part()

    def step(k, _):
        @pl.when((k > 0) & (k + 1 < chunks))
        def _():
            reduce_part(k + 1)

        @pl.when((k == inside) & (dp % 2 == 0))
        def _():
            cross_last(0).start()
            cross_last(1).start()

        owner_part(k)

        @pl.when((k >= 2) & (k < inside + 1))
        def _():
            cross(k - 2).wait_recv()

            @pl.when(k >= RING + 2)
            def _():
                forward(k - RING - 2).wait_send()

            forward(k - 2).start()

        @pl.when(k >= 2)
        def _():
            give(k - 2).wait_recv()

        @pl.when(k >= 4)
        def _():
            forward(k - 4).wait_recv()

    lax.fori_loop(0, chunks, step, None)

    @pl.when(dp % 2 == 0)
    def _():
        cross_last(0).wait_send()
        pl.semaphore_signal(turn, inc=1, device_id=(rep, partner), device_id_type=MESH)

    @pl.when(dp % 2 == 1)
    def _():
        pl.semaphore_wait(turn, 1)
        cross_last(0).start()
        cross_last(1).start()
        cross_last(0).wait_send()

    tail = lb.shape[0]
    la[:quarter] = out[chunks - 2, rows(dp)]
    la[quarter:] = out[chunks - 1, rows(dp, 0, quarter - tail)]
    lb[...] = out[chunks - 1, rows(dp, quarter - tail, tail)]

    for k in range(chunks - 2, chunks):
        for i in range(2):
            term(k, i).wait_send()
        half(k).wait_send()

    for k in range(chunks - RING, chunks):
        give(k).wait_send()
    for k in range(chunks - 2, chunks):
        give(k).wait_recv()
    for k in range(inside - 1 - RING, inside - 1):
        cross(k).wait_send()
        forward(k).wait_send()
    for k in range(chunks - 4, inside - 1):
        forward(k).wait_recv()
    cross_last(0).wait_recv()
    cross_last(1).wait()


def write(done, out, sem):
    chunks = done.shape[0]
    per = chunks // out.shape[0]

    def copy(k):
        return pltpu.make_async_copy(done.at[k], out.at[k // per, :, pl.ds((k % per) * WIDTH, WIDTH)], sem.at[k])

    for k in range(chunks):
        copy(k).start()
    for k in range(chunks):
        copy(k).wait()


def patch(spots, *refs):
    parts, out, sem = refs[:-3], refs[-2], refs[-1]
    _, dim, wide = out.shape
    per = wide // WIDTH
    dp = lax.axis_index("dp")
    copies = []
    for i, pieces in enumerate(spots):
        start = 0
        for k, row, size in pieces:
            for j, q in enumerate(((dp + 2) % 4, 3 - dp)):
                rows = pl.ds(pl.multiple_of(q * (dim // 4) + row, 128), size)
                copies.append(pltpu.make_async_copy(
                    parts[2 * i + j].at[pl.ds(start, size)],
                    out.at[k // per, rows, pl.ds((k % per) * WIDTH, WIDTH)], sem.at[len(copies)]))
            start += size
    for copy in copies:
        copy.start()
    for copy in copies:
        copy.wait()


def solution(mesh):
    def step(a, g):
        _, mats, tokens, dim = a.shape
        wide = g.shape[3]
        chunks = mats * (wide // WIDTH)
        block = (dim // 4, WIDTH)
        dma = pltpu.SemaphoreType.DMA
        bf16, f32 = jnp.bfloat16, jnp.float32
        quarter = dim // 4
        done, got, la, lb = pl.pallas_call(
            kernel,
            out_shape=tuple(pltpu.VMEM(shape, bf16) for shape in (
                (chunks, dim, WIDTH), block, (2 * quarter - TAIL, WIDTH), (TAIL, WIDTH))),
            in_specs=[pl.BlockSpec(memory_space=pl.ANY)] * 2,
            out_specs=(pl.BlockSpec(memory_space=pltpu.VMEM),) * 4,
            scratch_shapes=[
                pltpu.VMEM((tokens, dim), bf16),
                pltpu.VMEM((3, tokens, WIDTH), bf16),
                pltpu.VMEM((2, 2, *block), bf16),
                pltpu.VMEM((2, 2, *block), bf16),
                pltpu.VMEM(block, f32),
                pltpu.VMEM((2, *block), bf16),
                pltpu.VMEM((RING, *block), bf16),
                dma((4,)), dma((2, 2)), dma((3,)), dma((2,)), dma((2, 2)),
                dma((2, 2)), dma((2, 2)), dma((4,)),
                dma((2,)), dma((RING,)),
                dma((RING,)), dma((RING,)),
                dma((RING,)), dma((RING,)),
                dma((RING,)), dma((RING,)), dma((2,)), dma((2,)), pltpu.SemaphoreType.REGULAR,
            ],
            compiler_params=pltpu.CompilerParams(
                collective_id=0, has_side_effects=True, vmem_limit_bytes=38_000_000),
            name="reduce",
        )(a, g)

        def across(x):
            return lax.ppermute(x, "dp", [(d, (d + 2) % 4) for d in range(4)])

        def beside(x):
            return lax.ppermute(x, "dp", [(d, d ^ 1) for d in range(4)])

        def patched(out, spots, *parts):
            return pl.pallas_call(
                functools.partial(patch, spots),
                out_shape=jax.ShapeDtypeStruct(out.shape, out.dtype),
                in_specs=[pl.BlockSpec(memory_space=pltpu.VMEM)] * len(parts) + [pl.BlockSpec(memory_space=pl.ANY)],
                out_specs=pl.BlockSpec(memory_space=pl.ANY),
                input_output_aliases={len(parts): 0},
                scratch_shapes=[dma((2 * sum(len(s) for s in spots),))],
                compiler_params=pltpu.CompilerParams(vmem_limit_bytes=1_000_000),
            )(*parts, out)

        near_a = across(la)
        near_b = across(lb)
        got_far = beside(got)
        out = pl.pallas_call(
            write,
            out_shape=jax.ShapeDtypeStruct((mats, dim, wide), bf16),
            in_specs=[pl.BlockSpec(memory_space=pltpu.VMEM)],
            out_specs=pl.BlockSpec(memory_space=pl.ANY),
            scratch_shapes=[dma((chunks,))],
            compiler_params=pltpu.CompilerParams(vmem_limit_bytes=1_000_000),
            name="write",
        )(done)
        far_a = beside(near_a)
        far_b = beside(near_b)
        end = chunks - 1
        out = patched(
            out, (((end - 2, 0, quarter),), ((end - 1, 0, quarter), (end, 0, quarter - TAIL))),
            got, got_far, near_a, far_a)
        return patched(out, (((end, quarter - TAIL, TAIL),),), near_b, far_b)

    both = P(("rep", "dp"))
    return jax.shard_map(step, mesh=mesh, in_specs=(both, both), out_specs=P("rep"), check_vma=False)
```

```python
import functools

import jax
import jax.numpy as jnp
from jax import lax
from jax.experimental import pallas as pl
from jax.experimental.pallas import tpu as pltpu
from jax.sharding import PartitionSpec as P


MESH = pl.DeviceIdType.MESH
WIDTH = 640
RING = 4
SPLIT = 192
PIECES = ((0, 0, 128, 0, 256), (0, 128, 128, 0, 256), (0, 0, 128, 256, 384), (0, 128, 128, 256, 384), (1, 0, 128, 0, 640), (1, 128, 128, 0, 640))
LAST = 2
TAIL = 128


def kernel(
    a, g, out, got, la, lb, abuf, gbuf, sb1, rv1, total, sb2, rv2,
    asem, hsem, gsem, g0sem, ksem, s1, r1, q1, s2, r2, s3, r3, s4, r4, s5, r5, s6, r6, turn,
):
    _, mats, tokens, dim = a.shape
    quarter = dim // 4
    per = g.shape[3] // WIDTH
    chunks = mats * per
    inside = chunks - LAST
    rep, dp = lax.axis_index("rep"), lax.axis_index("dp")
    partner = 2 * (dp // 2) + 1 - dp % 2
    peer = (dp + 2) % 4
    order = (3 - dp, partner, peer, dp)

    def rows(q, start=0, size=quarter):
        return pl.ds(pl.multiple_of(q * quarter + start, 128), size)

    def columns(k):
        return pl.ds(pl.multiple_of((k % per) * WIDTH, 128), WIDTH)

    def place(k, q):
        return out.at[k, rows(q)]

    def load_a(n, i):
        return pltpu.make_async_copy(
            a.at[0, n, :, rows(order[i])], abuf.at[:, rows(order[i])], asem.at[i])

    def load_half(i, h):
        part = rows(order[i], h * 128, 128)
        return pltpu.make_async_copy(a.at[0, 0, :, part], abuf.at[:, part], hsem.at[i // 2, h])

    def load_first_a(j):
        deep, part = pl.ds(j * (tokens // 4), tokens // 4), rows(order[0], 0, 128)
        return pltpu.make_async_copy(a.at[0, 0, deep, part], abuf.at[deep, part], ksem.at[0, j])

    def load_first_g(j):
        deep, part = pl.ds(j * (tokens // 4), tokens // 4), pl.ds(0, 256)
        return pltpu.make_async_copy(g.at[0, 0, deep, part], gbuf.at[0, deep, part], ksem.at[1, j])

    def load_g(k):
        return pltpu.make_async_copy(g.at[0, k // per, :, columns(k)], gbuf.at[k % 3], gsem.at[k % 3])

    def load_g0(j, start, size):
        part = pl.ds(start, size)
        return pltpu.make_async_copy(g.at[0, 0, :, part], gbuf.at[0, :, part], g0sem.at[j])

    def remote(src, dst, send, recv, to):
        return pltpu.make_async_remote_copy(
            src_ref=src, dst_ref=dst, send_sem=send, recv_sem=recv,
            device_id=(rep, to), device_id_type=MESH)

    def term(k, i):
        return remote(sb1.at[k % 2, i], rv1.at[k % 2, i], s1.at[k % 2, i], r1.at[k % 2, i], partner)

    def term_piece(j):
        k, r, h, c, w = PIECES[j]
        part = (pl.ds(r, h), pl.ds(c, w))
        return remote(sb1.at[k, 0, *part], rv1.at[k, 0, *part], s1.at[k, 0], q1.at[j % 4], partner)

    def half(k):
        return remote(sb2.at[k % 2], rv2.at[k % RING], s2.at[k % 2], r2.at[k % RING], peer)

    def half_piece(j):
        k, r, h, c, w = PIECES[j]
        part = (pl.ds(r, h), pl.ds(c, w))
        return remote(sb2.at[k, *part], rv2.at[k, *part], s2.at[k], r2.at[k], peer)

    def give(k):
        return remote(place(k, dp), place(k, dp), s3.at[k % RING], r3.at[k % RING], partner)

    def cross(k):
        return remote(place(k, dp), place(k, dp), s4.at[k % RING], r4.at[k % RING], peer)

    def cross_last(j):
        start, size = ((0, SPLIT), (SPLIT, quarter - SPLIT))[j]
        return remote(out.at[inside - 1, pl.ds(pl.multiple_of(dp * quarter + start, 16), size)],
                      got.at[pl.ds(start, size)], s6.at[j], r6.at[j], peer)

    def forward(k):
        return remote(place(k, peer), place(k, peer), s5.at[k % RING], r5.at[k % RING], partner)

    def dot(left, right):
        return lax.dot_general(left, right, (((0,), (0,)), ((), ())), preferred_element_type=jnp.float32)

    def product(k, i):
        return dot(abuf[:, rows(order[i])], gbuf[k % 3])

    def both(here, there):
        return here + there.astype(jnp.float32)

    def first_part():
        def piece(j, i):
            k, r, h, c, w = PIECES[j]
            return dot(abuf[:, rows(order[i], r, h)], gbuf[k, :, c:c + w])

        def send(j):
            k, r, h, c, w = PIECES[j]
            term_piece(j).wait_recv()
            sb2[k, r:r + h, c:c + w] = both(total[r:r + h, c:c + w], rv1[k, 0, r:r + h, c:c + w]).astype(jnp.bfloat16)
            half_piece(j).start()

        waited = set()

        def need(name, load, *args):
            if name not in waited:
                waited.add(name)
                load(*args).wait()

        for j, (k, r, h, c, w) in enumerate(PIECES):
            halves = [x for x in range(2) if k == 0 and r < (x + 1) * 128 and r + h > x * 128]
            if j == 0:
                for d in range(4):
                    load_first_a(d).wait()
                    load_first_g(d).wait()
                    deep = slice(d * (tokens // 4), (d + 1) * (tokens // 4))
                    part = dot(abuf[deep, rows(order[0], 0, 128)], gbuf[0, deep, :256])
                    total[:128, :256] = part if d == 0 else total[:128, :256] + part
            elif k == 0:
                for x in halves:
                    if x:
                        need((0, x), load_half, 0, x)
            if k == 0 and c + w > 256:
                need("h", load_g0, 1, 256, 384)
            if k == 1:
                need("k", load_g, 1)
            own = total[:128, :256] if j == 0 else piece(j, 0)
            sb1[k, 0, r:r + h, c:c + w] = own.astype(jnp.bfloat16)
            if j == 0:
                pl.semaphore_wait(pltpu.get_barrier_semaphore(), 2)
            term_piece(j).start()
            if j:
                send(j - 1)
            for x in halves:
                need((2, x), load_half, 2, x)
            total[r:r + h, c:c + w] = piece(j, 2)
            if j == 0:
                load_g(1).start()
                load_a(0, 1).start()
                load_a(0, 3).start()
        send(len(PIECES) - 1)
        load_g(2).start()

    def next_a(k, i):
        @pl.when((k % per == per - 1) & (k + 1 < chunks))
        def _():
            load_a(k // per + 1, i).start()
            load_a(k // per + 1, i + 2).start()

    def reduce_part(k):
        first = k % per == 0
        load_g(k).wait()

        @pl.when(first)
        def _():
            load_a(k // per, 0).wait()
            load_a(k // per, 2).wait()

        term(k - 2, 0).wait_send()

        sb1[k % 2, 0] = product(k, 0).astype(jnp.bfloat16)
        term(k, 0).start()
        total[...] = product(k, 2)
        next_a(k, 0)
        term(k, 0).wait_recv()

        half(k - 2).wait_send()

        sb2[k % 2] = both(total[...], rv1[k % 2, 0]).astype(jnp.bfloat16)
        half(k).start()

    def owner_part(k):
        @pl.when(k % per == 0)
        def _():
            load_a(k // per, 1).wait()
            load_a(k // per, 3).wait()

        @pl.when(k >= 2)
        def _():
            term(k - 2, 1).wait_send()

        sb1[k % 2, 1] = product(k, 1).astype(jnp.bfloat16)
        term(k, 1).start()
        total[...] = product(k, 3)

        @pl.when(k + 3 < chunks)
        def _():
            load_g(k + 3).start()

        next_a(k, 1)
        term(k, 1).wait_recv()

        half(k).wait_recv()

        out[k, rows(dp)] = both(both(total[...], rv1[k % 2, 1]), rv2[k % RING]).astype(jnp.bfloat16)

        @pl.when((k >= RING) & (k < inside - 1))
        def _():
            cross(k - RING).wait_send()

        @pl.when(k < inside - 1)
        def _():
            cross(k).start()

        @pl.when(k >= RING)
        def _():
            give(k - RING).wait_send()

        give(k).start()

    for j in range(4):
        load_first_a(j).start()
        load_first_g(j).start()
    load_half(2, 0).start()
    load_half(0, 1).start()
    load_half(2, 1).start()
    load_g0(1, 256, 384).start()
    barrier = pltpu.get_barrier_semaphore()
    for other in (partner, peer):
        pl.semaphore_signal(barrier, inc=1, device_id=(rep, other), device_id_type=MESH)
    first_part()

    def step(k, _):
        @pl.when((k > 0) & (k + 1 < chunks))
        def _():
            reduce_part(k + 1)

        @pl.when((k == inside) & (dp % 2 == 0))
        def _():
            cross_last(0).start()
            cross_last(1).start()

        owner_part(k)

        @pl.when((k >= 2) & (k < inside + 1))
        def _():
            cross(k - 2).wait_recv()

            @pl.when(k >= RING + 2)
            def _():
                forward(k - RING - 2).wait_send()

            forward(k - 2).start()

        @pl.when(k >= 2)
        def _():
            give(k - 2).wait_recv()

        @pl.when(k >= 4)
        def _():
            forward(k - 4).wait_recv()

    lax.fori_loop(0, chunks, step, None)

    @pl.when(dp % 2 == 0)
    def _():
        cross_last(0).wait_send()
        pl.semaphore_signal(turn, inc=1, device_id=(rep, partner), device_id_type=MESH)

    @pl.when(dp % 2 == 1)
    def _():
        pl.semaphore_wait(turn, 1)
        cross_last(0).start()
        cross_last(1).start()
        cross_last(0).wait_send()

    tail = lb.shape[0]
    la[:quarter] = out[chunks - 2, rows(dp)]
    la[quarter:] = out[chunks - 1, rows(dp, 0, quarter - tail)]
    lb[...] = out[chunks - 1, rows(dp, quarter - tail, tail)]

    for k in range(chunks - 2, chunks):
        for i in range(2):
            term(k, i).wait_send()
        half(k).wait_send()

    for k in range(chunks - RING, chunks):
        give(k).wait_send()
    for k in range(chunks - 2, chunks):
        give(k).wait_recv()
    for k in range(inside - 1 - RING, inside - 1):
        cross(k).wait_send()
        forward(k).wait_send()
    for k in range(chunks - 4, inside - 1):
        forward(k).wait_recv()
    cross_last(0).wait_recv()
    cross_last(1).wait()


def write(done, out, sem):
    chunks = done.shape[0]
    per = chunks // out.shape[0]

    def copy(k):
        return pltpu.make_async_copy(done.at[k], out.at[k // per, :, pl.ds((k % per) * WIDTH, WIDTH)], sem.at[k])

    for k in range(chunks):
        copy(k).start()
    for k in range(chunks):
        copy(k).wait()


def patch(spots, *refs):
    parts, out, sem = refs[:-3], refs[-2], refs[-1]
    _, dim, wide = out.shape
    per = wide // WIDTH
    dp = lax.axis_index("dp")
    copies = []
    for i, pieces in enumerate(spots):
        start = 0
        for k, row, size in pieces:
            for j, q in enumerate(((dp + 2) % 4, 3 - dp)):
                rows = pl.ds(pl.multiple_of(q * (dim // 4) + row, 128), size)
                copies.append(pltpu.make_async_copy(
                    parts[2 * i + j].at[pl.ds(start, size)],
                    out.at[k // per, rows, pl.ds((k % per) * WIDTH, WIDTH)], sem.at[len(copies)]))
            start += size
    for copy in copies:
        copy.start()
    for copy in copies:
        copy.wait()


def solution(mesh):
    def step(a, g):
        _, mats, tokens, dim = a.shape
        wide = g.shape[3]
        chunks = mats * (wide // WIDTH)
        block = (dim // 4, WIDTH)
        dma = pltpu.SemaphoreType.DMA
        bf16, f32 = jnp.bfloat16, jnp.float32
        quarter = dim // 4
        done, got, la, lb = pl.pallas_call(
            kernel,
            out_shape=tuple(pltpu.VMEM(shape, bf16) for shape in (
                (chunks, dim, WIDTH), block, (2 * quarter - TAIL, WIDTH), (TAIL, WIDTH))),
            in_specs=[pl.BlockSpec(memory_space=pl.ANY)] * 2,
            out_specs=(pl.BlockSpec(memory_space=pltpu.VMEM),) * 4,
            scratch_shapes=[
                pltpu.VMEM((tokens, dim), bf16),
                pltpu.VMEM((3, tokens, WIDTH), bf16),
                pltpu.VMEM((2, 2, *block), bf16),
                pltpu.VMEM((2, 2, *block), bf16),
                pltpu.VMEM(block, f32),
                pltpu.VMEM((2, *block), bf16),
                pltpu.VMEM((RING, *block), bf16),
                dma((4,)), dma((2, 2)), dma((3,)), dma((2,)), dma((2, 4)),
                dma((2, 2)), dma((2, 2)), dma((4,)),
                dma((2,)), dma((RING,)),
                dma((RING,)), dma((RING,)),
                dma((RING,)), dma((RING,)),
                dma((RING,)), dma((RING,)), dma((2,)), dma((2,)), pltpu.SemaphoreType.REGULAR,
            ],
            compiler_params=pltpu.CompilerParams(
                collective_id=0, has_side_effects=True, vmem_limit_bytes=38_000_000),
            name="reduce",
        )(a, g)

        def across(x):
            return lax.ppermute(x, "dp", [(d, (d + 2) % 4) for d in range(4)])

        def beside(x):
            return lax.ppermute(x, "dp", [(d, d ^ 1) for d in range(4)])

        def patched(out, spots, *parts):
            return pl.pallas_call(
                functools.partial(patch, spots),
                out_shape=jax.ShapeDtypeStruct(out.shape, out.dtype),
                in_specs=[pl.BlockSpec(memory_space=pltpu.VMEM)] * len(parts) + [pl.BlockSpec(memory_space=pl.ANY)],
                out_specs=pl.BlockSpec(memory_space=pl.ANY),
                input_output_aliases={len(parts): 0},
                scratch_shapes=[dma((2 * sum(len(s) for s in spots),))],
                compiler_params=pltpu.CompilerParams(vmem_limit_bytes=1_000_000),
            )(*parts, out)

        near_a = across(la)
        near_b = across(lb)
        got_far = beside(got)
        out = pl.pallas_call(
            write,
            out_shape=jax.ShapeDtypeStruct((mats, dim, wide), bf16),
            in_specs=[pl.BlockSpec(memory_space=pltpu.VMEM)],
            out_specs=pl.BlockSpec(memory_space=pl.ANY),
            scratch_shapes=[dma((chunks,))],
            compiler_params=pltpu.CompilerParams(vmem_limit_bytes=1_000_000),
            name="write",
        )(done)
        far_a = beside(near_a)
        far_b = beside(near_b)
        end = chunks - 1
        out = patched(
            out, (((end - 2, 0, quarter),), ((end - 1, 0, quarter), (end, 0, quarter - TAIL))),
            got, got_far, near_a, far_a)
        return patched(out, (((end, quarter - TAIL, TAIL),),), near_b, far_b)

    both = P(("rep", "dp"))
    return jax.shard_map(step, mesh=mesh, in_specs=(both, both), out_specs=P("rep"), check_vma=False)
```
